32 devices in a mesh: grp: 2 (over x), pix: 16 (over z, y, core).
Axes of the slice: x: 2, y: 2, z: 4, core: 2. Of those that a mesh axis runs over, the one named last changes fastest.
Arguments:
- slcs: bfloat16 [2, 2048, 2048], P(None, ('grp', 'pix')), parts along dimension 1, may hold values from -6 to 6
- ref_date: int32 [2], P('grp'), parts along dimension 0, may hold values from 0 to 15
Outputs:
- spectrum: float32 [2, 2048, 2048], P(None, ('grp', 'pix')), parts along dimension 1
- compressed: float32 [2, 64, 4096], P(None, None, ('grp', 'pix')), parts along dimension 2
The draws below stay inside these ranges and needn't reach their ends.
There are 2 independent parts, one for each index of `grp`. The reference program is written for one: setup_inputs(seed, part) draws one part's arguments, and reference() takes and returns one part's arrays. A program takes and returns all parts, laid end to end along the dimension named above; each array names one. Nothing has to cross between parts.
All inputs are finite; a program needn't handle non-finite values.
Results may differ from the reference program's by a relative error of at most 0.0057.
Values may be sent and summed in bfloat16 or wider, within the bound.
A program may use at most 64 MiB of HBM per device.

```python
import math
import jax
import jax.numpy as jnp
from jax import lax

DATES = 16
ROWS = 64
COLS_DEV = 128
HALF_X = 5
HALF_Y = 2
POWER_ITERS = 6
COLS = 2048
N_PIX = 16


def shard_levels(key, shape, split, smallest, top_value):
    def one(dim, parts):
        draws = jax.random.uniform(jax.random.fold_in(jax.random.fold_in(key, 6), dim), (parts,), jnp.float32, smallest / len(split), top_value / len(split))
        return jnp.repeat(jnp.exp(draws), shape[dim] // parts).reshape((-1,) + (1,) * (len(shape) - dim - 1))

    level = one(*split[0])
    for cut in split[1:]:
        level = level * one(*cut)
    return level


def normal_values(stream_key, shape, deviation, limit, shards=(), kind=jnp.bfloat16):
    entries = deviation * jax.random.normal(stream_key, shape, jnp.float32)
    if shards:
        entries = entries * shard_levels(stream_key, shape, shards, -0.22, 0.18)
    return jnp.clip(entries, -limit, limit).astype(kind)


def setup_inputs(seed: int = 0, part: int = 0) -> dict:
    seeds = jax.random.split(jax.random.key(seed), 3)
    part_keys = jax.random.split(jax.random.fold_in(seeds[2], part), 3)
    return {
        "slcs": normal_values(part_keys[0], (2, DATES * ROWS, COLS), 1.0, 6.0, ((1, 16),)),
        "ref_date": jax.random.randint(part_keys[1], (1,), 0, DATES).astype(jnp.int32),
    }


LOADING = 0.25

def window_counts(line_count, column_count, first_column, strip_columns, half_lines, half_columns):
    line_index = jnp.arange(line_count, dtype=jnp.int32)
    column_index = first_column + jnp.arange(column_count, dtype=jnp.int32)
    line_span = jnp.minimum(line_index + half_lines, line_count - 1) - jnp.maximum(line_index - half_lines, 0) + 1
    column_span = jnp.minimum(column_index + half_columns, strip_columns - 1) - jnp.maximum(column_index - half_columns, 0) + 1
    return line_span.astype(jnp.float32)[:, None] * column_span.astype(jnp.float32)[None, :]

def box_window(products, column_count, half_lines, half_columns):
    summed = products[..., 0:column_count]
    for offset in range(1, 2 * half_columns + 1):
        summed = summed + products[..., offset:offset + column_count]
    line_count = summed.shape[-2]
    widths = [(0, 0)] * (summed.ndim - 2) + [(half_lines, half_lines), (0, 0)]
    padded = jnp.pad(summed, widths)
    result = padded[..., 0:line_count, :]
    for offset in range(1, 2 * half_lines + 1):
        result = result + padded[..., offset:offset + line_count, :]
    return result

def tile_covariance(window_data, counts, column_count):
    real_part = window_data[0]
    imag_part = window_data[1]

    def one_date(date_index):
        real_one = lax.dynamic_index_in_dim(real_part, date_index, 0, keepdims=True)
        imag_one = lax.dynamic_index_in_dim(imag_part, date_index, 0, keepdims=True)
        product_real = real_one * real_part + imag_one * imag_part
        product_imag = imag_one * real_part - real_one * imag_part
        stacked = jnp.stack([product_real, product_imag])
        return (box_window(stacked, column_count, HALF_Y, HALF_X) / counts).astype(jnp.bfloat16)
    return lax.map(one_date, jnp.arange(real_part.shape[0], dtype=jnp.int32))

def dct_table(line_count):
    frequency = jnp.arange(line_count, dtype=jnp.float32)[:, None]
    position = jnp.arange(line_count, dtype=jnp.float32)[None, :]
    weight = jnp.where(frequency == 0, math.sqrt(1.0 / line_count), math.sqrt(2.0 / line_count))
    return weight * jnp.cos(jnp.pi * (2.0 * position + 1.0) * frequency / (2.0 * line_count))

def process_tile(window_bf16, first_column, strip_columns, reference_date):
    window_data = window_bf16.astype(jnp.float32)
    column_count = window_data.shape[3] - 2 * HALF_X
    line_count = window_data.shape[2]
    counts = window_counts(line_count, column_count, first_column, strip_columns, HALF_Y, HALF_X)
    covariance = tile_covariance(window_data, counts, column_count)
    date_count = covariance.shape[0]
    pick = (jnp.arange(date_count, dtype=jnp.int32) == reference_date).astype(jnp.float32)[:, None, None]
    start_real = jnp.broadcast_to(pick, (date_count, line_count, column_count))
    start_imag = jnp.zeros_like(start_real)

    def power_step(step_index, vector):
        vec_real, vec_imag = vector
        cov_real = covariance[:, 0].astype(jnp.float32)
        cov_imag = covariance[:, 1].astype(jnp.float32)
        new_real = lax.optimization_barrier(jnp.sum(cov_real * vec_real[None] - cov_imag * vec_imag[None], axis=1)) + LOADING * vec_real
        new_imag = lax.optimization_barrier(jnp.sum(cov_real * vec_imag[None] + cov_imag * vec_real[None], axis=1)) + LOADING * vec_imag
        length = jnp.sqrt(lax.optimization_barrier(jnp.sum(new_real * new_real + new_imag * new_imag, axis=0)))
        return (new_real / length, new_imag / length)
    vec_real, vec_imag = lax.fori_loop(0, POWER_ITERS, power_step, (start_real, start_imag))
    ref_real = lax.optimization_barrier(jnp.sum(vec_real * pick, axis=0))
    ref_imag = lax.optimization_barrier(jnp.sum(vec_imag * pick, axis=0))
    linked_real = DATES * (vec_real * ref_real + vec_imag * ref_imag)
    linked_imag = DATES * (vec_imag * ref_real - vec_real * ref_imag)
    center = window_data[..., HALF_X:HALF_X + column_count]
    scaling = 1.0 / math.sqrt(DATES)
    comp_real = lax.optimization_barrier(jnp.sum(linked_real * center[0] + linked_imag * center[1], axis=0)) * scaling
    comp_imag = lax.optimization_barrier(jnp.sum(linked_real * center[1] - linked_imag * center[0], axis=0)) * scaling
    linked_stack = jnp.stack([linked_real, linked_imag])
    table = dct_table(line_count)
    transformed = jnp.einsum('qr,pkrc->pkqc', table, linked_stack, precision=lax.Precision.HIGHEST)
    spectrum_tile = transformed.reshape(2, date_count * line_count, column_count)
    return (spectrum_tile, jnp.stack([comp_real, comp_imag]))

def reference(slcs, ref_date):
    stacked_data = slcs.reshape(2, DATES, ROWS, COLS)
    padded = jnp.pad(stacked_data, ((0, 0), (0, 0), (0, 0), (HALF_X, HALF_X)))

    def one_tile(tile_index):
        first_column = (tile_index * COLS_DEV).astype(jnp.int32)
        window_bf16 = lax.dynamic_slice_in_dim(padded, first_column, COLS_DEV + 2 * HALF_X, 3)
        return process_tile(window_bf16, first_column, COLS, ref_date[0])
    spectra, compressed_tiles = lax.map(one_tile, jnp.arange(N_PIX, dtype=jnp.int32))
    spectrum = jnp.transpose(spectra, (1, 2, 0, 3)).reshape(2, DATES * ROWS, COLS)
    compressed = jnp.transpose(compressed_tiles, (1, 2, 0, 3)).reshape(2, ROWS, COLS)
    return (spectrum, compressed)
```

```python
import functools
import math

import jax
import jax.numpy as jnp
import numpy as np
from jax import lax
from jax.experimental import pallas as pl
from jax.experimental.pallas import tpu as pltpu
from jax.sharding import PartitionSpec as P

DATES = 16
ROWS = 64
HALF_X = 5
HALF_Y = 2
POWER_ITERS = 6
LOADING = 0.25

LANES = 128
SUB = 8
GROUPS = ROWS // SUB
HALO = LANES // GROUPS
REACH = DATES // 2
PLANES = 2 * (REACH + 1) - 1
MESH = pl.DeviceIdType.MESH


def line_order():
    return np.array([s * GROUPS + g for g in range(GROUPS) for s in range(SUB)])


def window_weights(columns):
    source = np.arange(columns)[:, None]
    target = np.arange(columns)[None, :]
    band = (np.abs(source - target) <= HALF_X).astype(np.float32)
    halo_column = np.concatenate([np.arange(-HALF_X, 0), columns + np.arange(HALF_X)])
    halo_band = np.zeros((HALO, columns), np.float32)
    halo_band[: 2 * HALF_X] = np.abs(halo_column[:, None] - target) <= HALF_X
    wide = np.zeros((GROUPS, HALO, GROUPS, columns), np.float32)
    for g in range(GROUPS):
        wide[g, :, g] = halo_band
    wide = wide.reshape(GROUPS * HALO, GROUPS // 2, 2 * columns).transpose(1, 0, 2)
    twice = np.concatenate([band, band], axis=0)
    wide_twice = np.concatenate([wide, wide], axis=1)
    return jnp.asarray(twice, jnp.bfloat16), jnp.asarray(wide_twice, jnp.bfloat16)


def dct_weights():
    frequency = np.arange(ROWS, dtype=np.float64)[:, None]
    position = np.arange(ROWS, dtype=np.float64)[None, :]
    weight = np.where(frequency == 0, math.sqrt(1.0 / ROWS), math.sqrt(2.0 / ROWS))
    table = weight * np.cos(np.pi * (2.0 * position + 1.0) * frequency / (2.0 * ROWS))
    table = table[:, line_order()].astype(np.float32)
    high = table.astype(jnp.bfloat16)
    low = (table - high.astype(np.float32)).astype(jnp.bfloat16)
    return jnp.asarray(np.concatenate([high, low, high], axis=1))


def greet(devices, me):
    barrier = pltpu.get_barrier_semaphore()
    for off in range(1, devices):
        pl.semaphore_signal(
            barrier, inc=1, device_id={"pix": lax.rem(me + off, devices)}, device_id_type=MESH
        )
    pl.semaphore_wait(barrier, devices - 1)


def gather_kernel(devices, x_ref, h_ref, w_ref, hw_ref, ssem, rsem, hs, hr, own):
    me = lax.axis_index("pix")
    columns = w_ref.shape[3]

    def block(d):
        return x_ref.at[:, :, pl.ds(pl.multiple_of(d * columns, columns), columns)]

    local = [
        pltpu.make_async_copy(block(me), w_ref.at[me], own.at[0]),
        pltpu.make_async_copy(h_ref.at[me], hw_ref.at[me], own.at[1]),
    ]
    for c in local:
        c.start()
    greet(devices, me)
    copies = []
    for off in range(1, devices):
        peer = lax.rem(me + off, devices)
        for src, dst, s, r in (
            (block(peer), w_ref.at[me], ssem, rsem),
            (h_ref.at[peer], hw_ref.at[me], hs, hr),
        ):
            c = pltpu.make_async_remote_copy(
                src_ref=src, dst_ref=dst, send_sem=s.at[off], recv_sem=r.at[off],
                device_id={"pix": peer}, device_id_type=MESH,
            )
            c.start()
            copies.append(c)
    for c in local + copies:
        c.wait()


def scatter_kernel(devices, t_ref, o_ref, ssem, rsem, own):
    me = lax.axis_index("pix")
    columns = t_ref.shape[3]
    mine = o_ref.at[:, :, pl.ds(pl.multiple_of(me * columns, columns), columns)]
    local = pltpu.make_async_copy(t_ref.at[me], mine, own)
    local.start()
    greet(devices, me)
    copies = [local]
    for off in range(1, devices):
        peer = lax.rem(me + off, devices)
        c = pltpu.make_async_remote_copy(
            src_ref=t_ref.at[peer], dst_ref=mine, send_sem=ssem.at[off], recv_sem=rsem.at[off],
            device_id={"pix": peer}, device_id_type=MESH,
        )
        c.start()
        copies.append(c)
    for c in copies:
        c.wait()


def split_halves(value):
    high = value.astype(jnp.bfloat16)
    low = (value - high.astype(jnp.float32)).astype(jnp.bfloat16)
    return high, low


def pair_products(read, i):
    real_one, imag_one = read(i, 0), read(i, 1)
    planes = [real_one * real_one + imag_one * imag_one]
    for d in range(1, REACH + 1):
        j = lax.rem(i + d, DATES)
        real_two, imag_two = read(j, 0), read(j, 1)
        planes.append(real_one * real_two + imag_one * imag_two)
        planes.append(imag_one * real_two - real_one * imag_two)
    return planes


def plane_of(d, part):
    return 0 if d == 0 else 2 * d - 1 + part


def link_kernel(strip_columns, ref_ref, w_ref, hw_ref, band_ref, wide_ref, dct_ref,
                spec_ref, comp_ref,
                stage, zf, hz, lhs_h, out_h, lhs, summed, inv, cov, vec, linked, comp):
    columns = w_ref.shape[3]
    first_column = lax.axis_index("pix") * columns
    sub = lax.broadcasted_iota(jnp.int32, (SUB, columns), 0)
    lane = lax.broadcasted_iota(jnp.int32, (SUB, columns), 1) + first_column
    across = jnp.minimum(lane + HALF_X, strip_columns - 1) - jnp.maximum(lane - HALF_X, 0) + 1
    for g in range(GROUPS):
        line = sub * GROUPS + g
        along = jnp.minimum(line + HALF_Y, ROWS - 1) - jnp.maximum(line - HALF_Y, 0) + 1
        inv[g] = 1.0 / (along * across).astype(jnp.float32)

    def prepare(k, carry):
        halo = hw_ref[k].astype(jnp.float32)
        for c in range(2):
            stage[c] = w_ref[k, c].astype(jnp.float32)
            hz[k, c] = halo[c * SUB:(c + 1) * SUB]
        for c in range(2):
            for g in range(GROUPS):
                zf[k, c, g] = stage[c, pl.ds(g, SUB, stride=GROUPS), :]
        return carry

    lax.fori_loop(0, DATES, prepare, 0)

    def halo_products(i, carry):
        planes = pair_products(lambda k, c: hz[k, c], i)
        planes.append(jnp.zeros_like(planes[0]))
        high, low = split_halves(jnp.concatenate(planes, axis=0))
        at = pl.ds(pl.multiple_of(i * (PLANES + 1) * SUB, 16), (PLANES + 1) * SUB)
        lhs_h[at, 0:LANES] = high
        lhs_h[at, LANES:2 * LANES] = low
        return carry

    lax.fori_loop(0, DATES, halo_products, 0)

    def halo_sums(n, carry):
        got = jnp.dot(lhs_h[...], wide_ref[n], preferred_element_type=jnp.float32)
        out_h[2 * n] = got[:, 0:columns]
        out_h[2 * n + 1] = got[:, columns:2 * columns]
        return carry

    lax.fori_loop(0, GROUPS // 2, halo_sums, 0)

    def covariances(i, carry):
        planes = pair_products(lambda k, c: zf[k, c].reshape(ROWS, columns), i)
        for p, value in enumerate(planes):
            high, low = split_halves(value)
            lhs[p * ROWS:(p + 1) * ROWS, 0:columns] = high
            lhs[p * ROWS:(p + 1) * ROWS, columns:2 * columns] = low
        summed[...] = jnp.dot(lhs[...], band_ref[...], preferred_element_type=jnp.float32)
        for d in range(REACH + 1):
            for part in range(1 if d == 0 else 2):
                p = plane_of(d, part)
                row = pl.multiple_of((i * (PLANES + 1) + p) * SUB, SUB)
                rows = [
                    summed[(p * GROUPS + g) * SUB:(p * GROUPS + g + 1) * SUB]
                    + out_h[g, pl.ds(row, SUB), :]
                    for g in range(GROUPS)
                ]
                before = [
                    jnp.where(sub == 0, 0.0, pltpu.roll(x, 1, 0)) for x in rows[-HALF_Y:]
                ]
                after = [
                    jnp.where(sub == SUB - 1, 0.0, pltpu.roll(x, SUB - 1, 0))
                    for x in rows[:HALF_Y]
                ]
                ext = before + rows + after
                two = [ext[q] + ext[q + 1] for q in range(GROUPS + 2)]
                for g in range(GROUPS):
                    value = (two[g] + two[g + 2] + ext[g + 4]) * inv[g]
                    if d == 0:
                        value = value + LOADING
                    cov[i, p, g] = value
        return carry

    lax.fori_loop(0, DATES, covariances, 0)

    ref = ref_ref[0]

    def solve(g, carry):
        for i in range(DATES):
            d = lax.rem(ref - i + DATES, DATES)
            fwd = d <= REACH
            dd = jnp.where(fwd, d, DATES - d)
            one = jnp.where(fwd, i, ref)
            pr = jnp.maximum(2 * dd - 1, 0)
            sign = jnp.where(d == 0, 0.0, jnp.where(fwd, 1.0, -1.0))
            vec[0, i, 0] = cov[one, pr, g]
            vec[0, i, 1] = cov[one, 2 * dd, g] * sign

        def step(t, carry):
            src = lax.rem(t, 2)
            for base in range(0, DATES, 8):
                real = [None] * 8
                imag = [None] * 8
                for j in range(DATES):
                    vr, vi = vec[src, j, 0], vec[src, j, 1]
                    for q in range(8):
                        i = base + q
                        d = (j - i) % DATES
                        if d == 0:
                            cr = cov[i, 0, g]
                            add_r, add_i = cr * vr, cr * vi
                        elif d <= REACH:
                            cr, ci = cov[i, 2 * d - 1, g], cov[i, 2 * d, g]
                            add_r, add_i = cr * vr - ci * vi, cr * vi + ci * vr
                        else:
                            d = DATES - d
                            cr, ci = cov[j, 2 * d - 1, g], cov[j, 2 * d, g]
                            add_r, add_i = cr * vr + ci * vi, cr * vi - ci * vr
                        real[q] = add_r if real[q] is None else real[q] + add_r
                        imag[q] = add_i if imag[q] is None else imag[q] + add_i
                for q in range(8):
                    vec[1 - src, base + q, 0] = real[q]
                    vec[1 - src, base + q, 1] = imag[q]
            return carry

        lax.fori_loop(0, POWER_ITERS - 1, step, 0)
        last = (POWER_ITERS - 1) % 2
        total = jnp.zeros((SUB, columns), jnp.float32)
        for k in range(DATES):
            vr, vi = vec[last, k, 0], vec[last, k, 1]
            total = total + (vr * vr + vi * vi)
        scale = DATES / total
        rr, ri = vec[last, ref, 0] * scale, vec[last, ref, 1] * scale
        comp_r = jnp.zeros_like(total)
        comp_i = jnp.zeros_like(total)
        at = pl.ds(pl.multiple_of(g * SUB, SUB), SUB)
        for k in range(DATES):
            vr, vi = vec[last, k, 0], vec[last, k, 1]
            lr = vr * rr + vi * ri
            li = vi * rr - vr * ri
            zr, zi = zf[k, 0, g], zf[k, 1, g]
            comp_r = comp_r + (lr * zr + li * zi)
            comp_i = comp_i + (lr * zi - li * zr)
            linked[k, at, 0:columns] = lr
            linked[k, at, columns:2 * columns] = li
        comp[0, g] = comp_r * (1.0 / math.sqrt(DATES))
        comp[1, g] = comp_i * (1.0 / math.sqrt(DATES))
        return carry

    lax.fori_loop(0, GROUPS, solve, 0)
    for c in range(2):
        for g in range(GROUPS):
            comp_ref[c, pl.ds(g, SUB, stride=GROUPS), :] = comp[c, g]

    def transform(k, carry):
        high, low = split_halves(linked[k])
        both = jnp.concatenate([high, high, low], axis=0)
        got = jnp.dot(dct_ref[...], both, preferred_element_type=jnp.float32)
        got = got.astype(spec_ref.dtype)
        spec_ref[k, 0] = got[:, 0:columns]
        spec_ref[k, 1] = got[:, columns:2 * columns]
        return carry

    lax.fori_loop(0, DATES, transform, 0)


def link_call(strip_columns, ref_date, window, halo):
    columns = window.shape[3]
    band, wide = window_weights(columns)
    f32, bf16 = jnp.float32, jnp.bfloat16
    vmem = pl.BlockSpec(memory_space=pltpu.VMEM)
    return pl.pallas_call(
        functools.partial(link_kernel, strip_columns),
        out_shape=(
            jax.ShapeDtypeStruct((DATES, 2, ROWS, columns), bf16),
            jax.ShapeDtypeStruct((2, ROWS, columns), f32),
        ),
        in_specs=[pl.BlockSpec(memory_space=pltpu.SMEM)] + [vmem] * 5,
        out_specs=(vmem, vmem),
        scratch_shapes=[
            pltpu.VMEM((2, ROWS, columns), f32),
            pltpu.VMEM((DATES, 2, GROUPS, SUB, columns), f32),
            pltpu.VMEM((DATES, 2, SUB, LANES), f32),
            pltpu.VMEM((DATES * (PLANES + 1) * SUB, 2 * LANES), bf16),
            pltpu.VMEM((GROUPS, DATES * (PLANES + 1) * SUB, columns), f32),
            pltpu.VMEM((PLANES * ROWS, 2 * columns), bf16),
            pltpu.VMEM((PLANES * ROWS, columns), f32),
            pltpu.VMEM((GROUPS, SUB, columns), f32),
            pltpu.VMEM((DATES, PLANES, GROUPS, SUB, columns), f32),
            pltpu.VMEM((2, DATES, 2, SUB, columns), f32),
            pltpu.VMEM((DATES, ROWS, 2 * columns), f32),
            pltpu.VMEM((2, GROUPS, SUB, columns), f32),
        ],
        compiler_params=pltpu.CompilerParams(vmem_limit_bytes=56 * 1024 * 1024),
        name="link",
    )(ref_date, window, halo, band, wide, dct_weights())


def on_device(slcs, ref_date):
    devices = lax.axis_size("pix")
    local_rows, strip_columns = slcs.shape[1], slcs.shape[2]
    columns = strip_columns // devices
    per_date = ROWS // local_rows
    lines = local_rows // GROUPS
    pad_rows = max(16, 2 * lines)

    cut = slcs.reshape(2, local_rows, devices, columns)
    edge = jnp.zeros((2, local_rows, 1, HALF_X), slcs.dtype)
    left = jnp.concatenate([edge, cut[:, :, :-1, columns - HALF_X:]], axis=2)
    right = jnp.concatenate([cut[:, :, 1:, :HALF_X], edge], axis=2)
    fill = jnp.zeros((2, local_rows, devices, HALO - 2 * HALF_X), slcs.dtype)
    halo = jnp.concatenate([left, right, fill], axis=3)
    halo = halo.reshape(2, lines, GROUPS, devices, HALO).transpose(3, 0, 1, 2, 4)
    halo = halo.reshape(devices, 2 * lines, LANES)
    halo = jnp.pad(halo, ((0, 0), (0, pad_rows - 2 * lines), (0, 0)))

    anywhere = pl.BlockSpec(memory_space=pl.ANY)
    sems = pltpu.SemaphoreType.DMA((devices,))
    window, halo = pl.pallas_call(
        functools.partial(gather_kernel, devices),
        out_shape=(
            jax.ShapeDtypeStruct((devices, 2, local_rows, columns), slcs.dtype),
            jax.ShapeDtypeStruct(halo.shape, slcs.dtype),
        ),
        in_specs=[anywhere] * 2,
        out_specs=(anywhere, anywhere),
        scratch_shapes=[sems] * 4 + [pltpu.SemaphoreType.DMA((2,))],
        compiler_params=pltpu.CompilerParams(collective_id=0, has_side_effects=True),
        name="gather",
    )(slcs, halo)

    if per_date > 1:
        window = window.reshape(DATES, per_date, 2, local_rows, columns).transpose(0, 2, 1, 3, 4)
        halo = halo[:, :2 * lines].reshape(DATES, per_date, 2, lines, LANES)
        halo = halo.transpose(0, 2, 1, 3, 4)
    window = window.reshape(DATES, 2, ROWS, columns)
    halo = halo.reshape(DATES, 2 * SUB, LANES)

    tile, compressed = link_call(strip_columns, ref_date, window, halo)

    if per_date > 1:
        tile = tile.reshape(DATES, 2, per_date, local_rows, columns).transpose(0, 2, 1, 3, 4)
    tile = tile.reshape(devices, 2, local_rows, columns)
    spectrum = pl.pallas_call(
        functools.partial(scatter_kernel, devices),
        out_shape=jax.ShapeDtypeStruct((2, local_rows, strip_columns), tile.dtype),
        in_specs=[anywhere],
        out_specs=anywhere,
        scratch_shapes=[sems] * 2 + [pltpu.SemaphoreType.DMA],
        compiler_params=pltpu.CompilerParams(collective_id=1, has_side_effects=True),
        name="scatter",
    )(tile)
    return (spectrum.astype(jnp.float32), compressed)


def solution(mesh):
    return jax.shard_map(
        on_device,
        mesh=mesh,
        in_specs=(P(None, ("grp", "pix"), None), P("grp")),
        out_specs=(P(None, ("grp", "pix"), None), P(None, None, ("grp", "pix"))),
        check_vma=False,
    )
```

```python
import functools
import math

import jax
import jax.numpy as jnp
import numpy as np
from jax import lax
from jax.experimental import pallas as pl
from jax.experimental.pallas import tpu as pltpu
from jax.sharding import PartitionSpec as P

DATES = 16
ROWS = 64
HALF_X = 5
HALF_Y = 2
POWER_ITERS = 6
LOADING = 0.25

LANES = 128
SUB = 8
GROUPS = ROWS // SUB
HALO = LANES // GROUPS
CHUNK = 4
SPAN = 8
MESH = pl.DeviceIdType.MESH


def line_order():
    return np.array([s * GROUPS + g for g in range(GROUPS) for s in range(SUB)])


def window_weights(columns):
    source = np.arange(columns)[:, None]
    target = np.arange(columns)[None, :]
    band = (np.abs(source - target) <= HALF_X).astype(np.float32)
    halo_column = np.concatenate([np.arange(-HALF_X, 0), columns + np.arange(HALF_X)])
    halo_band = np.zeros((HALO, columns), np.float32)
    halo_band[: 2 * HALF_X] = np.abs(halo_column[:, None] - target) <= HALF_X
    wide = np.zeros((GROUPS, HALO, GROUPS, columns), np.float32)
    for g in range(GROUPS):
        wide[g, :, g] = halo_band
    wide = wide.reshape(GROUPS * HALO, GROUPS // 2, 2 * columns).transpose(1, 0, 2)
    twice = np.concatenate([band, band], axis=0)
    wide_twice = np.concatenate([wide, wide], axis=1)
    return jnp.asarray(twice, jnp.bfloat16), jnp.asarray(wide_twice, jnp.bfloat16)


def dct_weights():
    frequency = np.arange(ROWS, dtype=np.float64)[:, None]
    position = np.arange(ROWS, dtype=np.float64)[None, :]
    weight = np.where(frequency == 0, math.sqrt(1.0 / ROWS), math.sqrt(2.0 / ROWS))
    table = weight * np.cos(np.pi * (2.0 * position + 1.0) * frequency / (2.0 * ROWS))
    table = table[:, line_order()].astype(np.float32)
    high = table.astype(jnp.bfloat16)
    low = (table - high.astype(np.float32)).astype(jnp.bfloat16)
    return jnp.asarray(np.concatenate([high, low, high], axis=1))


def split_halves(value):
    high = value.astype(jnp.bfloat16)
    low = (value - high.astype(jnp.float32)).astype(jnp.bfloat16)
    return high, low


def pair_products(one, two):
    real = one[0] * two[0] + one[1] * two[1]
    imag = one[1] * two[0] - one[0] * two[1]
    return real, imag


def chunk_index(p):
    whole, rest = p // CHUNK, p % CHUNK
    return (whole + 1) * (whole * (CHUNK // 2) + rest)


def link_kernel(devices, ref_ref, h_ref, x_ref, band_ref, wide_ref, dct_ref,
                o_ref, comp_ref,
                xs, win, hwin, band, wide, dct, stage, zf, hz, lhs_h, out_h, lhs, summed, inv,
                cov, vec, linked, comp, tile,
                local, ssem, rsem, hs, hr, ts, tr):
    columns = win.shape[3]
    local_rows = win.shape[2]
    strip_columns = x_ref.shape[2]
    per_date = ROWS // local_rows
    lines = local_rows // GROUPS
    me = lax.axis_index("pix")
    my_date = me // per_date

    loads = [
        pltpu.make_async_copy(src, dst, local.at[n])
        for n, (src, dst) in enumerate(
            ((x_ref, xs), (wide_ref, wide), (band_ref, band), (dct_ref, dct))
        )
    ]
    for load in loads:
        load.start()
    barrier = pltpu.get_barrier_semaphore()
    for off in range(1, devices):
        pl.semaphore_signal(
            barrier, inc=1, device_id={"pix": lax.rem(me + off, devices)}, device_id_type=MESH
        )

    first_column = me * columns
    sub = lax.broadcasted_iota(jnp.int32, (SUB, columns), 0)
    lane = lax.broadcasted_iota(jnp.int32, (SUB, columns), 1) + first_column
    across = jnp.minimum(lane + HALF_X, strip_columns - 1) - jnp.maximum(lane - HALF_X, 0) + 1
    for g in range(GROUPS):
        line = sub * GROUPS + g
        along = jnp.minimum(line + HALF_Y, ROWS - 1) - jnp.maximum(line - HALF_Y, 0) + 1
        inv[g] = 1.0 / (along * across).astype(jnp.float32)

    pl.semaphore_wait(barrier, devices - 1)
    loads[0].wait()

    def block(n):
        return xs.at[:, :, pl.ds(pl.multiple_of(n * columns, columns), columns)]

    def main_copy(off):
        peer = lax.rem(me + off, devices)
        return pltpu.make_async_remote_copy(
            src_ref=block(peer), dst_ref=win.at[me], send_sem=ssem.at[off], recv_sem=rsem.at[off],
            device_id={"pix": peer}, device_id_type=MESH,
        )

    def halo_copy(off):
        peer = lax.rem(me + off, devices)
        return pltpu.make_async_remote_copy(
            src_ref=h_ref.at[peer], dst_ref=hwin.at[me], send_sem=hs.at[off],
            recv_sem=hr.at[off], device_id={"pix": peer}, device_id_type=MESH,
        )

    halos = [halo_copy(off) for off in range(1, devices)]
    mains = [main_copy(off) for off in range(1, devices)]
    for c in halos + mains:
        c.start()
    own = [
        pltpu.make_async_copy(block(me), win.at[me], local.at[4]),
        pltpu.make_async_copy(h_ref.at[me], hwin.at[me], local.at[5]),
    ]
    for c in own:
        c.start()
    for c in own + loads[1:] + halos:
        c.wait()

    def date_at(p):
        return lax.rem(my_date - p + DATES, DATES)

    def prepare_halo(p, carry):
        for q in range(per_date):
            halo = hwin[date_at(p) * per_date + q].astype(jnp.float32)
            for c in range(2):
                hz[p, c, q * lines:(q + 1) * lines] = halo[c * lines:(c + 1) * lines]
        return carry

    lax.fori_loop(0, DATES, prepare_halo, 0)

    def halo_products(p, carry):
        one = hz[p, 0], hz[p, 1]

        def chunk(n, carry):
            planes = []
            for q in range(CHUNK):
                planes += pair_products(one, (hz[n * CHUNK + q, 0], hz[n * CHUNK + q, 1]))
            high, low = split_halves(jnp.concatenate(planes, axis=0))
            size = 2 * CHUNK * SUB
            at = pl.ds(pl.multiple_of((chunk_index(p) + n) * size, size), size)
            lhs_h[at, 0:LANES] = high
            lhs_h[at, LANES:2 * LANES] = low
            return carry

        return lax.fori_loop(0, p // CHUNK + 1, chunk, carry)

    lax.fori_loop(0, DATES, halo_products, 0)

    def halo_sums(n, carry):
        got = jnp.dot(lhs_h[...], wide[n], preferred_element_type=jnp.float32)
        out_h[2 * n] = got[:, 0:columns]
        out_h[2 * n + 1] = got[:, columns:2 * columns]
        return carry

    lax.fori_loop(0, GROUPS // 2, halo_sums, 0)

    def window_sums(row, first):
        rows = [
            summed[first + g * SUB:first + (g + 1) * SUB] + out_h[g, pl.ds(row, SUB), :]
            for g in range(GROUPS)
        ]
        before = [jnp.where(sub == 0, 0.0, pltpu.roll(x, 1, 0)) for x in rows[-HALF_Y:]]
        after = [jnp.where(sub == SUB - 1, 0.0, pltpu.roll(x, SUB - 1, 0)) for x in rows[:HALF_Y]]
        ext = before + rows + after
        two = [ext[g] + ext[g + 1] for g in range(GROUPS + 2)]
        return [(two[g] + two[g + 2] + ext[g + 4]) * inv[g] for g in range(GROUPS)]

    def covariances(p, carry):
        for q in range(per_date):
            source = date_at(p) * per_date + q
            off = lax.rem(me - source + devices, devices)

            @pl.when(off != 0)
            def _():
                main_copy(off).wait_recv()

            for c in range(2):
                stage[c, q * local_rows:(q + 1) * local_rows] = win[source, c].astype(jnp.float32)
        for c in range(2):
            for g in range(GROUPS):
                zf[p, c, g] = stage[c, pl.ds(g, SUB, stride=GROUPS), :]

        def chunk(n, carry):
            one = zf[p, 0].reshape(ROWS, columns), zf[p, 1].reshape(ROWS, columns)
            for q in range(CHUNK):
                k = n * CHUNK + q
                two = zf[k, 0].reshape(ROWS, columns), zf[k, 1].reshape(ROWS, columns)
                for part, value in enumerate(pair_products(one, two)):
                    high, low = split_halves(value)
                    at = (2 * q + part) * ROWS
                    lhs[at:at + ROWS, 0:columns] = high
                    lhs[at:at + ROWS, columns:2 * columns] = low
            summed[...] = jnp.dot(lhs[...], band[...], preferred_element_type=jnp.float32)
            size = 2 * CHUNK * SUB
            base = (chunk_index(p) + n) * size
            for q in range(CHUNK):
                sums = [
                    window_sums(
                        pl.multiple_of(base + (2 * q + part) * SUB, SUB), (2 * q + part) * ROWS
                    )
                    for part in range(2)
                ]
                for g in range(GROUPS):
                    real, imag = sums[0][g], sums[1][g]
                    cov[p, n * CHUNK + q, 0, g] = real
                    cov[p, n * CHUNK + q, 1, g] = real + imag
                    cov[p, n * CHUNK + q, 2, g] = imag - real
            return carry

        lax.fori_loop(0, p // CHUNK + 1, chunk, 0)
        for g in range(GROUPS):
            cov[p, p, 0, g] = cov[p, p, 0, g] + LOADING
        return carry

    lax.fori_loop(0, DATES, covariances, 0)

    ref = lax.rem(my_date - ref_ref[0] + DATES, DATES)

    def solve(g, carry):
        for i in range(DATES):
            one, two = jnp.maximum(ref, i), jnp.minimum(ref, i)
            real = cov[one, two, 0, g]
            imag = 0.5 * (cov[one, two, 1, g] + cov[one, two, 2, g])
            sign = jnp.where(ref == i, 0.0, jnp.where(ref < i, 1.0, -1.0))
            imag = imag * sign
            vec[0, i, 0] = real
            vec[0, i, 1] = imag
            vec[0, i, 2] = real + imag

        def step(t, carry):
            src = lax.rem(t, 2)
            for base in range(0, DATES, SPAN):
                acc = [[None] * 3 for _ in range(SPAN)]
                for j in range(DATES):
                    vr, vi, vs = vec[src, j, 0], vec[src, j, 1], vec[src, j, 2]
                    for q in range(SPAN):
                        i = base + q
                        one, two = max(i, j), min(i, j)
                        cr = cov[one, two, 0, g]
                        if i == j:
                            terms = (cr * vs, cr * vi, -(cr * vr))
                        elif i > j:
                            terms = (cr * vs, cov[i, j, 1, g] * vi, cov[i, j, 2, g] * vr)
                        else:
                            terms = (cr * vs, -(cov[j, i, 2, g] * vi), -(cov[j, i, 1, g] * vr))
                        for n in range(3):
                            acc[q][n] = terms[n] if acc[q][n] is None else acc[q][n] + terms[n]
                for q in range(SPAN):
                    real, imag = acc[q][0] - acc[q][1], acc[q][0] + acc[q][2]
                    vec[1 - src, base + q, 0] = real
                    vec[1 - src, base + q, 1] = imag
                    vec[1 - src, base + q, 2] = real + imag
            return carry

        lax.fori_loop(0, POWER_ITERS - 1, step, 0)
        last = (POWER_ITERS - 1) % 2
        total = jnp.zeros((SUB, columns), jnp.float32)
        for k in range(DATES):
            vr, vi = vec[last, k, 0], vec[last, k, 1]
            total = total + (vr * vr + vi * vi)
        scale = DATES / total
        rr, ri = vec[last, ref, 0] * scale, vec[last, ref, 1] * scale
        comp_r = jnp.zeros_like(total)
        comp_i = jnp.zeros_like(total)
        at = pl.ds(pl.multiple_of(g * SUB, SUB), SUB)
        for k in range(DATES):
            vr, vi = vec[last, k, 0], vec[last, k, 1]
            lr = vr * rr + vi * ri
            li = vi * rr - vr * ri
            zr, zi = zf[k, 0, g], zf[k, 1, g]
            comp_r = comp_r + (lr * zr + li * zi)
            comp_i = comp_i + (lr * zi - li * zr)
            linked[k, at, 0:columns] = lr
            linked[k, at, columns:2 * columns] = li
        comp[0, g] = comp_r * (1.0 / math.sqrt(DATES))
        comp[1, g] = comp_i * (1.0 / math.sqrt(DATES))
        return carry

    lax.fori_loop(0, GROUPS, solve, 0)

    mine = o_ref.at[:, :, pl.ds(pl.multiple_of(first_column, columns), columns)]

    def tile_copy(p, q):
        peer = date_at(p) * per_date + q
        off = lax.rem(peer - me + devices, devices)
        return off, pltpu.make_async_remote_copy(
            src_ref=tile.at[p, :, q * local_rows:(q + 1) * local_rows, :], dst_ref=mine,
            send_sem=ts.at[off], recv_sem=tr.at[off],
            device_id={"pix": peer}, device_id_type=MESH,
        )

    def send(p):
        for q in range(per_date):
            off, copy = tile_copy(p, q)

            @pl.when(off != 0)
            def _():
                copy.start()

            @pl.when(off == 0)
            def _():
                pltpu.make_async_copy(
                    tile.at[p, :, q * local_rows:(q + 1) * local_rows, :], mine, local.at[6]
                ).start()

    def transform(p, carry):
        high, low = split_halves(linked[p])
        both = jnp.concatenate([high, high, low], axis=0)
        got = jnp.dot(dct[...], both, preferred_element_type=jnp.float32).astype(tile.dtype)
        tile[p, 0] = got[:, 0:columns]
        tile[p, 1] = got[:, columns:2 * columns]

        @pl.when(p > 0)
        def _():
            send(p - 1)

        return carry

    lax.fori_loop(0, DATES, transform, 0)
    for c in range(2):
        for g in range(GROUPS):
            comp_ref[c, pl.ds(g, SUB, stride=GROUPS), :] = comp[c, g]
    send(DATES - 1)

    for c in mains:
        c.wait_send()
    own_tile = tile.at[0, :, 0:local_rows, :]
    pltpu.make_async_copy(own_tile, mine, local.at[6]).wait()
    for off in range(1, devices):
        pltpu.make_async_remote_copy(
            src_ref=own_tile, dst_ref=mine, send_sem=ts.at[off], recv_sem=tr.at[off],
            device_id={"pix": lax.rem(me + off, devices)}, device_id_type=MESH,
        ).wait()


def on_device(slcs, ref_date):
    devices = lax.axis_size("pix")
    local_rows, strip_columns = slcs.shape[1], slcs.shape[2]
    columns = strip_columns // devices
    per_date = ROWS // local_rows
    lines = local_rows // GROUPS
    pad_rows = max(16, 2 * lines)

    cut = slcs.reshape(2, local_rows, devices, columns)
    edge = jnp.zeros((2, local_rows, 1, HALF_X), slcs.dtype)
    left = jnp.concatenate([edge, cut[:, :, :-1, columns - HALF_X:]], axis=2)
    right = jnp.concatenate([cut[:, :, 1:, :HALF_X], edge], axis=2)
    fill = jnp.zeros((2, local_rows, devices, HALO - 2 * HALF_X), slcs.dtype)
    halo = jnp.concatenate([left, right, fill], axis=3)
    halo = halo.reshape(2, lines, GROUPS, devices, HALO).transpose(3, 0, 1, 2, 4)
    halo = halo.reshape(devices, 2 * lines, LANES)
    halo = jnp.pad(halo, ((0, 0), (0, pad_rows - 2 * lines), (0, 0)))

    anywhere = pl.BlockSpec(memory_space=pl.ANY)
    vmem = pl.BlockSpec(memory_space=pltpu.VMEM)
    band, wide = window_weights(columns)
    dct = dct_weights()
    f32, bf16 = jnp.float32, jnp.bfloat16
    halo_lines = chunk_index(DATES) * 2 * CHUNK * SUB
    sems = pltpu.SemaphoreType.DMA((devices,))
    spectrum, compressed = pl.pallas_call(
        functools.partial(link_kernel, devices),
        out_shape=(
            jax.ShapeDtypeStruct((2, local_rows, strip_columns), bf16),
            jax.ShapeDtypeStruct((2, ROWS, columns), f32),
        ),
        in_specs=[pl.BlockSpec(memory_space=pltpu.SMEM), vmem] + [anywhere] * 4,
        out_specs=(anywhere, vmem),
        scratch_shapes=[
            pltpu.VMEM(slcs.shape, bf16),
            pltpu.VMEM((devices, 2, local_rows, columns), bf16),
            pltpu.VMEM(halo.shape, bf16),
            pltpu.VMEM(band.shape, bf16),
            pltpu.VMEM(wide.shape, bf16),
            pltpu.VMEM(dct.shape, bf16),
            pltpu.VMEM((2, ROWS, columns), f32),
            pltpu.VMEM((DATES, 2, GROUPS, SUB, columns), f32),
            pltpu.VMEM((DATES, 2, SUB, LANES), f32),
            pltpu.VMEM((halo_lines, 2 * LANES), bf16),
            pltpu.VMEM((GROUPS, halo_lines, columns), f32),
            pltpu.VMEM((2 * CHUNK * ROWS, 2 * columns), bf16),
            pltpu.VMEM((2 * CHUNK * ROWS, columns), f32),
            pltpu.VMEM((GROUPS, SUB, columns), f32),
            pltpu.VMEM((DATES, DATES, 3, GROUPS, SUB, columns), f32),
            pltpu.VMEM((2, DATES, 3, SUB, columns), f32),
            pltpu.VMEM((DATES, ROWS, 2 * columns), f32),
            pltpu.VMEM((2, GROUPS, SUB, columns), f32),
            pltpu.VMEM((DATES, 2, ROWS, columns), bf16),
            pltpu.SemaphoreType.DMA((7,)),
        ] + [sems] * 6,
        compiler_params=pltpu.CompilerParams(
            collective_id=0, has_side_effects=True, vmem_limit_bytes=60 * 1024 * 1024
        ),
        name="link",
    )(ref_date, halo, slcs, band, wide, dct)
    return (spectrum.astype(jnp.float32), compressed)


def solution(mesh):
    return jax.shard_map(
        on_device,
        mesh=mesh,
        in_specs=(P(None, ("grp", "pix"), None), P("grp")),
        out_specs=(P(None, ("grp", "pix"), None), P(None, None, ("grp", "pix"))),
        check_vma=False,
    )
```

```python
import functools
import math

import jax
import jax.numpy as jnp
import numpy as np
from jax import lax
from jax.experimental import pallas as pl
from jax.experimental.pallas import tpu as pltpu
from jax.sharding import PartitionSpec as P

DATES = 16
ROWS = 64
HALF_X = 5
HALF_Y = 2
POWER_ITERS = 6
LOADING = 0.25

LANES = 128
SUB = 8
GROUPS = ROWS // SUB
HALO = LANES // GROUPS
CHUNK = 4
SPAN = 8
MESH = pl.DeviceIdType.MESH


def line_order():
    return np.array([s * GROUPS + g for g in range(GROUPS) for s in range(SUB)])


def window_weights(columns):
    source = np.arange(columns)[:, None]
    target = np.arange(columns)[None, :]
    band = (np.abs(source - target) <= HALF_X).astype(np.float32)
    halo_column = np.concatenate([np.arange(-HALF_X, 0), columns + np.arange(HALF_X)])
    halo_band = np.zeros((HALO, columns), np.float32)
    halo_band[: 2 * HALF_X] = np.abs(halo_column[:, None] - target) <= HALF_X
    wide = np.zeros((GROUPS, HALO, GROUPS, columns), np.float32)
    for g in range(GROUPS):
        wide[g, :, g] = halo_band
    wide = wide.reshape(GROUPS * HALO, GROUPS // 2, 2 * columns).transpose(1, 0, 2)
    twice = np.concatenate([band, band], axis=0)
    wide_twice = np.concatenate([wide, wide], axis=1)
    return jnp.asarray(twice, jnp.bfloat16), jnp.asarray(wide_twice, jnp.bfloat16)


def dct_weights():
    frequency = np.arange(ROWS, dtype=np.float64)[:, None]
    position = np.arange(ROWS, dtype=np.float64)[None, :]
    weight = np.where(frequency == 0, math.sqrt(1.0 / ROWS), math.sqrt(2.0 / ROWS))
    table = weight * np.cos(np.pi * (2.0 * position + 1.0) * frequency / (2.0 * ROWS))
    table = table[:, line_order()].astype(np.float32)
    high = table.astype(jnp.bfloat16)
    low = (table - high.astype(np.float32)).astype(jnp.bfloat16)
    return jnp.asarray(np.concatenate([high, low, high], axis=1))


def split_halves(value):
    high = value.astype(jnp.bfloat16)
    low = (value - high.astype(jnp.float32)).astype(jnp.bfloat16)
    return high, low


def pair_products(one, two):
    real = one[0] * two[0] + one[1] * two[1]
    imag = one[1] * two[0] - one[0] * two[1]
    return real, imag


def exclusive_or(a, b, size):
    total, bit = 0, 1
    while bit < size:
        total = total + ((a // bit + b // bit) % 2) * bit
        bit *= 2
    return total


def chunk_index(p):
    whole, rest = p // CHUNK, p % CHUNK
    return (whole + 1) * (whole * (CHUNK // 2) + rest)


def link_kernel(devices, ref_ref, h_ref, x_ref, band_ref, wide_ref, dct_ref,
                o_ref, comp_ref,
                xs, win, hwin, band, wide, dct, stage, zf, hz, lhs_h, out_h, lhs, summed, inv,
                cov, vec, linked, comp, tile,
                local, ssem, rsem, hs, hr, ts, tr):
    columns = win.shape[3]
    local_rows = win.shape[2]
    strip_columns = x_ref.shape[2]
    per_date = ROWS // local_rows
    lines = local_rows // GROUPS
    me = lax.axis_index("pix")
    my_date = me // per_date

    loads = [
        pltpu.make_async_copy(src, dst, local.at[n])
        for n, (src, dst) in enumerate(
            ((x_ref, xs), (wide_ref, wide), (band_ref, band), (dct_ref, dct))
        )
    ]
    for load in loads:
        load.start()
    barrier = pltpu.get_barrier_semaphore()
    for off in range(1, devices):
        pl.semaphore_signal(
            barrier, inc=1, device_id={"pix": exclusive_or(me, off, devices)}, device_id_type=MESH
        )

    first_column = me * columns
    sub = lax.broadcasted_iota(jnp.int32, (SUB, columns), 0)
    lane = lax.broadcasted_iota(jnp.int32, (SUB, columns), 1) + first_column
    across = jnp.minimum(lane + HALF_X, strip_columns - 1) - jnp.maximum(lane - HALF_X, 0) + 1
    for g in range(GROUPS):
        line = sub * GROUPS + g
        along = jnp.minimum(line + HALF_Y, ROWS - 1) - jnp.maximum(line - HALF_Y, 0) + 1
        inv[g] = 1.0 / (along * across).astype(jnp.float32)

    pl.semaphore_wait(barrier, devices - 1)
    loads[0].wait()

    def block(n):
        return xs.at[:, :, pl.ds(pl.multiple_of(n * columns, columns), columns)]

    def main_copy(off):
        peer = exclusive_or(me, off, devices)
        return pltpu.make_async_remote_copy(
            src_ref=block(peer), dst_ref=win.at[me], send_sem=ssem.at[off], recv_sem=rsem.at[off],
            device_id={"pix": peer}, device_id_type=MESH,
        )

    def halo_copy(off):
        peer = exclusive_or(me, off, devices)
        return pltpu.make_async_remote_copy(
            src_ref=h_ref.at[peer], dst_ref=hwin.at[me], send_sem=hs.at[off],
            recv_sem=hr.at[off], device_id={"pix": peer}, device_id_type=MESH,
        )

    halos = [halo_copy(off) for off in range(1, devices)]
    mains = [main_copy(off) for off in range(1, devices)]
    for c in halos + mains:
        c.start()
    own = [
        pltpu.make_async_copy(block(me), win.at[me], local.at[4]),
        pltpu.make_async_copy(h_ref.at[me], hwin.at[me], local.at[5]),
    ]
    for c in own:
        c.start()
    for c in own + loads[1:] + halos:
        c.wait()

    def date_at(p):
        return exclusive_or(my_date, p, DATES)

    def prepare_halo(p, carry):
        for q in range(per_date):
            halo = hwin[date_at(p) * per_date + q].astype(jnp.float32)
            for c in range(2):
                hz[p, c, q * lines:(q + 1) * lines] = halo[c * lines:(c + 1) * lines]
        return carry

    lax.fori_loop(0, DATES, prepare_halo, 0)

    def halo_products(p, carry):
        one = hz[p, 0], hz[p, 1]

        def chunk(n, carry):
            planes = []
            for q in range(CHUNK):
                planes += pair_products(one, (hz[n * CHUNK + q, 0], hz[n * CHUNK + q, 1]))
            high, low = split_halves(jnp.concatenate(planes, axis=0))
            size = 2 * CHUNK * SUB
            at = pl.ds(pl.multiple_of((chunk_index(p) + n) * size, size), size)
            lhs_h[at, 0:LANES] = high
            lhs_h[at, LANES:2 * LANES] = low
            return carry

        return lax.fori_loop(0, p // CHUNK + 1, chunk, carry)

    lax.fori_loop(0, DATES, halo_products, 0)

    def halo_sums(n, carry):
        got = jnp.dot(lhs_h[...], wide[n], preferred_element_type=jnp.float32)
        out_h[2 * n] = got[:, 0:columns]
        out_h[2 * n + 1] = got[:, columns:2 * columns]
        return carry

    lax.fori_loop(0, GROUPS // 2, halo_sums, 0)

    def window_sums(row, first):
        rows = [
            summed[first + g * SUB:first + (g + 1) * SUB] + out_h[g, pl.ds(row, SUB), :]
            for g in range(GROUPS)
        ]
        before = [jnp.where(sub == 0, 0.0, pltpu.roll(x, 1, 0)) for x in rows[-HALF_Y:]]
        after = [jnp.where(sub == SUB - 1, 0.0, pltpu.roll(x, SUB - 1, 0)) for x in rows[:HALF_Y]]
        ext = before + rows + after
        two = [ext[g] + ext[g + 1] for g in range(GROUPS + 2)]
        return [(two[g] + two[g + 2] + ext[g + 4]) * inv[g] for g in range(GROUPS)]

    def covariances(p, carry):
        for q in range(per_date):
            source = date_at(p) * per_date + q
            off = exclusive_or(me, source, devices)

            @pl.when(off != 0)
            def _():
                main_copy(off).wait_recv()

            for c in range(2):
                stage[c, q * local_rows:(q + 1) * local_rows] = win[source, c].astype(jnp.float32)
        for c in range(2):
            for g in range(GROUPS):
                zf[p, c, g] = stage[c, pl.ds(g, SUB, stride=GROUPS), :]

        def chunk(n, carry):
            one = zf[p, 0].reshape(ROWS, columns), zf[p, 1].reshape(ROWS, columns)
            for q in range(CHUNK):
                k = n * CHUNK + q
                two = zf[k, 0].reshape(ROWS, columns), zf[k, 1].reshape(ROWS, columns)
                for part, value in enumerate(pair_products(one, two)):
                    high, low = split_halves(value)
                    at = (2 * q + part) * ROWS
                    lhs[at:at + ROWS, 0:columns] = high
                    lhs[at:at + ROWS, columns:2 * columns] = low
            summed[...] = jnp.dot(lhs[...], band[...], preferred_element_type=jnp.float32)
            size = 2 * CHUNK * SUB
            base = (chunk_index(p) + n) * size
            for q in range(CHUNK):
                sums = [
                    window_sums(
                        pl.multiple_of(base + (2 * q + part) * SUB, SUB), (2 * q + part) * ROWS
                    )
                    for part in range(2)
                ]
                for g in range(GROUPS):
                    real, imag = sums[0][g], sums[1][g]
                    cov[g, p, n * CHUNK + q, 0] = real
                    cov[g, p, n * CHUNK + q, 1] = real + imag
                    cov[g, p, n * CHUNK + q, 2] = imag - real
            return carry

        lax.fori_loop(0, p // CHUNK + 1, chunk, 0)
        for g in range(GROUPS):
            cov[g, p, p, 0] = cov[g, p, p, 0] + LOADING
        return carry

    lax.fori_loop(0, DATES, covariances, 0)

    ref = exclusive_or(my_date, ref_ref[0], DATES)

    def solve(g, carry):
        for i in range(DATES):
            one, two = jnp.maximum(ref, i), jnp.minimum(ref, i)
            real = cov[g, one, two, 0]
            imag = 0.5 * (cov[g, one, two, 1] + cov[g, one, two, 2])
            sign = jnp.where(ref == i, 0.0, jnp.where(ref < i, 1.0, -1.0))
            imag = imag * sign
            vec[0, i, 0] = real
            vec[0, i, 1] = imag
            vec[0, i, 2] = real + imag

        def step(t, carry):
            src = lax.rem(t, 2)
            for base in range(0, DATES, SPAN):
                acc = [[None] * 3 for _ in range(SPAN)]
                for j in range(DATES):
                    vr, vi, vs = vec[src, j, 0], vec[src, j, 1], vec[src, j, 2]
                    for q in range(SPAN):
                        i = base + q
                        one, two = max(i, j), min(i, j)
                        cr = cov[g, one, two, 0]
                        if i == j:
                            terms, minus = (cr * vs, cr * vi, cr * vr), (False, False, True)
                        elif i > j:
                            terms = (cr * vs, cov[g, i, j, 1] * vi, cov[g, i, j, 2] * vr)
                            minus = (False, False, False)
                        else:
                            terms = (cr * vs, cov[g, j, i, 2] * vi, cov[g, j, i, 1] * vr)
                            minus = (False, True, True)
                        for n in range(3):
                            if acc[q][n] is None:
                                acc[q][n] = -terms[n] if minus[n] else terms[n]
                            elif minus[n]:
                                acc[q][n] = acc[q][n] - terms[n]
                            else:
                                acc[q][n] = acc[q][n] + terms[n]
                for q in range(SPAN):
                    real, imag = acc[q][0] - acc[q][1], acc[q][0] + acc[q][2]
                    vec[1 - src, base + q, 0] = real
                    vec[1 - src, base + q, 1] = imag
                    vec[1 - src, base + q, 2] = real + imag
            return carry

        lax.fori_loop(0, POWER_ITERS - 1, step, 0)
        last = (POWER_ITERS - 1) % 2
        total = jnp.zeros((SUB, columns), jnp.float32)
        for k in range(DATES):
            vr, vi = vec[last, k, 0], vec[last, k, 1]
            total = total + (vr * vr + vi * vi)
        scale = DATES / total
        rr, ri = vec[last, ref, 0] * scale, vec[last, ref, 1] * scale
        comp_r = jnp.zeros_like(total)
        comp_i = jnp.zeros_like(total)
        at = pl.ds(pl.multiple_of(g * SUB, SUB), SUB)
        for k in range(DATES):
            vr, vi = vec[last, k, 0], vec[last, k, 1]
            lr = vr * rr + vi * ri
            li = vi * rr - vr * ri
            zr, zi = zf[k, 0, g], zf[k, 1, g]
            comp_r = comp_r + (lr * zr + li * zi)
            comp_i = comp_i + (lr * zi - li * zr)
            linked[k, at, 0:columns] = lr
            linked[k, at, columns:2 * columns] = li
        comp[0, g] = comp_r * (1.0 / math.sqrt(DATES))
        comp[1, g] = comp_i * (1.0 / math.sqrt(DATES))
        return carry

    lax.fori_loop(0, GROUPS, solve, 0)

    mine = o_ref.at[:, :, pl.ds(pl.multiple_of(first_column, columns), columns)]

    def tile_copy(p, q):
        peer = date_at(p) * per_date + q
        off = exclusive_or(me, peer, devices)
        return off, pltpu.make_async_remote_copy(
            src_ref=tile.at[p, :, q * local_rows:(q + 1) * local_rows, :], dst_ref=mine,
            send_sem=ts.at[off], recv_sem=tr.at[off],
            device_id={"pix": peer}, device_id_type=MESH,
        )

    def send(p):
        for q in range(per_date):
            off, copy = tile_copy(p, q)

            @pl.when(off != 0)
            def _():
                copy.start()

            @pl.when(off == 0)
            def _():
                pltpu.make_async_copy(
                    tile.at[p, :, q * local_rows:(q + 1) * local_rows, :], mine, local.at[6]
                ).start()

    def transform(n, carry):
        p = DATES - 1 - n
        high, low = split_halves(linked[p])
        both = jnp.concatenate([high, high, low], axis=0)
        got = jnp.dot(dct[...], both, preferred_element_type=jnp.float32).astype(tile.dtype)
        tile[p, 0] = got[:, 0:columns]
        tile[p, 1] = got[:, columns:2 * columns]

        @pl.when(n > 0)
        def _():
            send(p + 1)

        return carry

    lax.fori_loop(0, DATES, transform, 0)
    for c in range(2):
        for g in range(GROUPS):
            comp_ref[c, pl.ds(g, SUB, stride=GROUPS), :] = comp[c, g]
    send(0)

    for c in mains:
        c.wait_send()
    own_tile = tile.at[0, :, 0:local_rows, :]
    pltpu.make_async_copy(own_tile, mine, local.at[6]).wait()
    for off in range(1, devices):
        pltpu.make_async_remote_copy(
            src_ref=own_tile, dst_ref=mine, send_sem=ts.at[off], recv_sem=tr.at[off],
            device_id={"pix": exclusive_or(me, off, devices)}, device_id_type=MESH,
        ).wait()


def on_device(slcs, ref_date):
    devices = lax.axis_size("pix")
    local_rows, strip_columns = slcs.shape[1], slcs.shape[2]
    columns = strip_columns // devices
    per_date = ROWS // local_rows
    lines = local_rows // GROUPS
    pad_rows = max(16, 2 * lines)

    cut = slcs.reshape(2, local_rows, devices, columns)
    edge = jnp.zeros((2, local_rows, 1, HALF_X), slcs.dtype)
    left = jnp.concatenate([edge, cut[:, :, :-1, columns - HALF_X:]], axis=2)
    right = jnp.concatenate([cut[:, :, 1:, :HALF_X], edge], axis=2)
    fill = jnp.zeros((2, local_rows, devices, HALO - 2 * HALF_X), slcs.dtype)
    halo = jnp.concatenate([left, right, fill], axis=3)
    halo = halo.reshape(2, lines, GROUPS, devices, HALO).transpose(3, 0, 1, 2, 4)
    halo = halo.reshape(devices, 2 * lines, LANES)
    halo = jnp.pad(halo, ((0, 0), (0, pad_rows - 2 * lines), (0, 0)))

    anywhere = pl.BlockSpec(memory_space=pl.ANY)
    vmem = pl.BlockSpec(memory_space=pltpu.VMEM)
    band, wide = window_weights(columns)
    dct = dct_weights()
    f32, bf16 = jnp.float32, jnp.bfloat16
    halo_lines = chunk_index(DATES) * 2 * CHUNK * SUB
    sems = pltpu.SemaphoreType.DMA((devices,))
    spectrum, compressed = pl.pallas_call(
        functools.partial(link_kernel, devices),
        out_shape=(
            jax.ShapeDtypeStruct((2, local_rows, strip_columns), bf16),
            jax.ShapeDtypeStruct((2, ROWS, columns), f32),
        ),
        in_specs=[pl.BlockSpec(memory_space=pltpu.SMEM), vmem] + [anywhere] * 4,
        out_specs=(anywhere, vmem),
        scratch_shapes=[
            pltpu.VMEM(slcs.shape, bf16),
            pltpu.VMEM((devices, 2, local_rows, columns), bf16),
            pltpu.VMEM(halo.shape, bf16),
            pltpu.VMEM(band.shape, bf16),
            pltpu.VMEM(wide.shape, bf16),
            pltpu.VMEM(dct.shape, bf16),
            pltpu.VMEM((2, ROWS, columns), f32),
            pltpu.VMEM((DATES, 2, GROUPS, SUB, columns), f32),
            pltpu.VMEM((DATES, 2, SUB, LANES), f32),
            pltpu.VMEM((halo_lines, 2 * LANES), bf16),
            pltpu.VMEM((GROUPS, halo_lines, columns), f32),
            pltpu.VMEM((2 * CHUNK * ROWS, 2 * columns), bf16),
            pltpu.VMEM((2 * CHUNK * ROWS, columns), f32),
            pltpu.VMEM((GROUPS, SUB, columns), f32),
            pltpu.VMEM((GROUPS, DATES, DATES, 3, SUB, columns), f32),
            pltpu.VMEM((2, DATES, 3, SUB, columns), f32),
            pltpu.VMEM((DATES, ROWS, 2 * columns), f32),
            pltpu.VMEM((2, GROUPS, SUB, columns), f32),
            pltpu.VMEM((DATES, 2, ROWS, columns), bf16),
            pltpu.SemaphoreType.DMA((7,)),
        ] + [sems] * 6,
        compiler_params=pltpu.CompilerParams(
            collective_id=0, has_side_effects=True, vmem_limit_bytes=60 * 1024 * 1024
        ),
        name="link",
    )(ref_date, halo, slcs, band, wide, dct)
    return (spectrum.astype(jnp.float32), compressed)


def solution(mesh):
    return jax.shard_map(
        on_device,
        mesh=mesh,
        in_specs=(P(None, ("grp", "pix"), None), P("grp")),
        out_specs=(P(None, ("grp", "pix"), None), P(None, None, ("grp", "pix"))),
        check_vma=False,
    )
```
